256 devices in a mesh: dp: 32 (over y_hi, z, core), tp: 8 (over x, y_lo).
Axes of the slice: x: 4, y: 4 (y_hi: 2, y_lo: 2; y = y_hi * 2 + y_lo), z: 8, core: 2. Of those that a mesh axis runs over, the one named last changes fastest.
Arguments:
- hidden: bfloat16 [32768, 4096], P(('dp', 'tp')), may hold values from -24 to 24
- query_grad: bfloat16 [32768, 4096], P('dp', 'tp'), may hold values from -1.5 to 1.5
- key_grad: bfloat16 [32768, 1024], P('dp', 'tp'), may hold values from -1.5 to 1.5
- value_grad: bfloat16 [32768, 1024], P('dp', 'tp'), may hold values from -1.5 to 1.5
- w_query: bfloat16 [4096, 4096], P(None, 'tp'), may hold values from -0.09375 to 0.09375
- w_key: bfloat16 [4096, 1024], P(None, 'tp'), may hold values from -0.09375 to 0.09375
- w_value: bfloat16 [4096, 1024], P(None, 'tp'), may hold values from -0.09375 to 0.09375
Outputs:
- hidden_grad: bfloat16 [32768, 4096], P(('dp', 'tp'))
- grad_query: float32 [4096, 4096], P('dp', 'tp')
- grad_key: float32 [4096, 1024], P('dp', 'tp')
- grad_value: float32 [4096, 1024], P('dp', 'tp')
The draws below stay inside these ranges and needn't reach their ends.
All inputs are finite; a program needn't handle non-finite values.
Results may differ from the reference program's by a relative error of at most 0.014.
Values may be sent and summed in bfloat16 or wider, within the bound.
No kernel may reach another device: no remote copies, remote signals or barrier semaphores. Data moves between devices by JAX's collectives and lax.ppermute only.
A program may use at most 256 MiB of HBM per device.

```python
import jax
import jax.numpy as jnp
from jax import lax

D = 4096
HEAD = 128
Q_DEV = 4
KV_HEADS = 8
Q_W = 4096
KV_W = 1024
GROUP_TOK = 1024
TOKENS = 32768
N_DP = 32


def raised(entries, key, source, target, blocks, factor):
    owner, partner = [(jnp.arange(entries.shape[position]) // (entries.shape[position] // blocks)).reshape([-1 if axis == position else 1 for axis in range(entries.ndim)]) for position in (source, target)]
    chosen = jax.random.permutation(key, blocks)[partner]
    strong = (owner == chosen) | (owner == (partner + blocks // 2) % blocks)
    return jnp.where(strong, factor * entries, entries)


def steps_of(stream_key, shape, shards, low, largest):
    gain, own = 1.0, jax.random.fold_in(stream_key, 6)
    for dim, blocks in shards:
        draws = jnp.exp(jax.random.uniform(jax.random.fold_in(own, dim), (blocks,), jnp.float32, low / len(shards), largest / len(shards)))
        gain = gain * jnp.repeat(draws, shape[dim] // blocks).reshape([-1 if axis == dim else 1 for axis in range(len(shape))])
    return gain


def gaussian(key, dims, scale, most, pieces=(), dtype=jnp.bfloat16):
    result = scale * jax.random.normal(key, dims, jnp.float32)
    if pieces:
        result = result * steps_of(key, dims, pieces, -0.22, 0.18)
    return jnp.clip(result, -most, most).astype(dtype)


def noise_with(stream_key, extent, scale, most, split, heavy, kind=jnp.bfloat16):
    array = scale * jax.random.normal(stream_key, extent, jnp.float32)
    if split:
        array = array * steps_of(stream_key, extent, split, -0.22, 0.18)
    return jnp.clip(raised(array, jax.random.fold_in(stream_key, 3), *heavy), -most, most).astype(kind)


def setup_inputs(seed: int = 0) -> dict:
    key_of = jax.random.split(jax.random.key(seed), 8)
    return {
        "hidden": noise_with(key_of[0], (TOKENS, D), 1.0, 24.0, ((0, 256),), (0, 1, 256, 6.0)),
        "query_grad": gaussian(key_of[1], (TOKENS, Q_W), 0.25, 1.5, ((0, 32), (1, 8))),
        "key_grad": gaussian(key_of[2], (TOKENS, KV_W), 0.25, 1.5, ((0, 32), (1, 8))),
        "value_grad": gaussian(key_of[3], (TOKENS, KV_W), 0.25, 1.5, ((0, 32), (1, 8))),
        "w_query": gaussian(key_of[4], (D, Q_W), D ** -0.5, 0.09375, ((1, 8),)),
        "w_key": gaussian(key_of[5], (D, KV_W), D ** -0.5, 0.09375, ((1, 8),)),
        "w_value": gaussian(key_of[6], (D, KV_W), D ** -0.5, 0.09375, ((1, 8),)),
    }


def contract_rows(left, right):
    return lax.dot_general(left, right, (((0,), (0,)), ((), ())), preferred_element_type=jnp.float32)


def rounded(value):
    return lax.optimization_barrier(value.astype(jnp.bfloat16)).astype(jnp.float32)


def reference(hidden, query_grad, key_grad, value_grad, w_query, w_key, w_value):
    hidden_groups = hidden.reshape(N_DP, GROUP_TOK, D)
    query_groups = query_grad.reshape(N_DP, GROUP_TOK, Q_W)
    key_groups = key_grad.reshape(N_DP, GROUP_TOK, KV_W)
    value_groups = value_grad.reshape(N_DP, GROUP_TOK, KV_W)
    weight_heads = jnp.concatenate((w_query.reshape(D, KV_HEADS, Q_DEV * HEAD), w_key.reshape(D, KV_HEADS, HEAD), w_value.reshape(D, KV_HEADS, HEAD)), axis=2).astype(jnp.float32)

    def one_group(totals, inputs):
        grad_wq, grad_wk, grad_wv = totals
        hid, qgr, kgr, vgr = inputs
        grad_heads = jnp.concatenate((qgr.reshape(GROUP_TOK, KV_HEADS, Q_DEV * HEAD), kgr.reshape(GROUP_TOK, KV_HEADS, HEAD), vgr.reshape(GROUP_TOK, KV_HEADS, HEAD)), axis=2).astype(jnp.float32)
        parts = jnp.einsum("thc,dhc->htd", grad_heads, weight_heads)
        hid_grad = jnp.sum(rounded(parts), axis=0).astype(jnp.bfloat16)
        grad_wq = grad_wq + rounded(contract_rows(hid, qgr))
        grad_wk = grad_wk + rounded(contract_rows(hid, kgr))
        grad_wv = grad_wv + rounded(contract_rows(hid, vgr))
        return (grad_wq, grad_wk, grad_wv), hid_grad

    zeros = (jnp.zeros((D, Q_W), jnp.float32), jnp.zeros((D, KV_W), jnp.float32), jnp.zeros((D, KV_W), jnp.float32))
    totals, outputs = lax.scan(one_group, zeros, (hidden_groups, query_groups, key_groups, value_groups))
    hidden_grad = outputs.reshape(TOKENS, D)
    return hidden_grad, totals[0], totals[1], totals[2]
```

```python
import jax
import jax.numpy as jnp
from jax import lax
from jax.sharding import Mesh
from jax.sharding import PartitionSpec as P
from jax.experimental import pallas as pl
from jax.experimental.pallas import tpu as pltpu


AXES = ("yh", "z", "c", "x", "yl")
DP = ("yh", "z", "c")
TP = ("x", "yl")
BF16 = jnp.bfloat16
F32 = jnp.float32


def swap(value, axis, partner, size):
    return lax.ppermute(value, axis, [(i, partner(i)) for i in range(size)])


def flip(i):
    return i ^ 1


def sequential(**limits):
    return pltpu.CompilerParams(dimension_semantics=("arbitrary",), **limits)


def cut(index, weights, piece):
    widths = [w.shape[1] for w in weights]
    cols = sum(widths)

    def body(index, *refs):
        at = 0
        for ref, width in zip(refs[:-1], widths, strict=True):
            refs[-1][:, at : at + width] = ref[...]
            at += width

    return pl.pallas_call(
        body,
        name="cut",
        out_shape=jax.ShapeDtypeStruct((piece, cols), BF16),
        grid_spec=pltpu.PrefetchScalarGridSpec(
            num_scalar_prefetch=1,
            grid=(1,),
            in_specs=[pl.BlockSpec((piece, w), lambda i, t: (t[0], 0)) for w in widths],
            out_specs=pl.BlockSpec((piece, cols), lambda i, t: (0, 0)),
        ),
        compiler_params=sequential(),
    )(index, *weights)


def ordered(table, grads, tok):
    widths = [g.shape[1] for g in grads]
    cols = sum(widths)
    n_rows = grads[0].shape[0]
    steps = n_rows // tok

    def body(table, *refs):
        ins, outs = refs[:3], refs[3:]
        for i in range(2 * steps):
            row = pl.multiple_of(table[i] * tok, tok)
            at = 0
            for k, width in enumerate(widths):
                to = (i % steps) * tok
                outs[i // steps][to : to + tok, at : at + width] = ins[k][pl.ds(row, tok), :]
                at += width

    out = jax.ShapeDtypeStruct((n_rows, cols), BF16)
    return pl.pallas_call(
        body,
        name="ordered",
        out_shape=[out, out],
        grid_spec=pltpu.PrefetchScalarGridSpec(
            num_scalar_prefetch=1,
            grid=(1,),
            in_specs=[pl.BlockSpec(g.shape, lambda i, t: (0, 0)) for g in grads],
            out_specs=[pl.BlockSpec((n_rows, cols), lambda i, t: (0, 0))] * 2,
        ),
        compiler_params=sequential(),
    )(table, *grads)


def input_product(table, at, mine, got, weights, pieces, others):
    widths = [w.shape[1] for w in weights]
    cols = sum(widths)
    n_rows = mine.shape[0] // 2
    piece = pieces.shape[0] // 4
    steps = 4

    def body(table, mine, got, q, k, v, pieces, others, upper, lower):
        left = jnp.concatenate((q[...], k[...], v[...]), axis=1)
        south = table[2 * steps] == 0
        first = jnp.where(south, pieces[...], others[...])
        second = jnp.where(south, others[...], pieces[...])
        right = jnp.concatenate((first, second), axis=0)

        def times(a, b):
            return lax.dot_general(
                a[...], b, (((1,), (1,)), ((), ())), preferred_element_type=F32
            )

        total = (times(mine, left) + times(got, right)).astype(BF16)
        upper[...] = total[: n_rows // 2]
        lower[...] = total[n_rows // 2 :]

    row_spec = pl.BlockSpec((n_rows, cols), lambda i, t: (at, 0))
    piece_spec = pl.BlockSpec((piece, cols), lambda i, t: (t[steps + i], 0))
    return pl.pallas_call(
        body,
        out_shape=[jax.ShapeDtypeStruct((n_rows // 2, steps * 2 * piece), BF16)] * 2,
        grid_spec=pltpu.PrefetchScalarGridSpec(
            num_scalar_prefetch=1,
            grid=(steps,),
            in_specs=[row_spec, row_spec]
            + [pl.BlockSpec((2 * piece, w), lambda i, t: (t[i], 0)) for w in widths]
            + [piece_spec, piece_spec],
            out_specs=[pl.BlockSpec((n_rows // 2, 2 * piece), lambda i, t: (0, i))] * 2,
        ),
        compiler_params=sequential(),
        cost_estimate=pl.CostEstimate(
            flops=8 * n_rows * steps * piece * cols,
            bytes_accessed=8 * steps * piece * cols,
            transcendentals=0,
        ),
    )(table, mine, got, *weights, pieces, others)


def dot_rows(left, right):
    return lax.dot_general(left, right, (((0,), (0,)), ((), ())), preferred_element_type=F32)


def joined(arrays):
    return jnp.concatenate(arrays, axis=0)


def body(hidden, query_grad, key_grad, value_grad, w_query, w_key, w_value):
    n_x = lax.axis_size("x")
    n_z = lax.axis_size("z")
    yl = lax.axis_index("yl")
    yh = lax.axis_index("yh")
    x = lax.axis_index("x")
    c = lax.axis_index("c")
    z = lax.axis_index("z")
    tok, width = hidden.shape
    half = width // 2
    q_cols, k_cols = w_query.shape[1], w_key.shape[1]
    cols = q_cols + 2 * k_cols
    last = n_x - 1
    weights = (w_query, w_key, w_value)

    def near(i):
        return i ^ 1

    def far(i):
        return last - i

    def z_near(i):
        return i ^ 1

    def z_far(i):
        return (i - 1 + 2 * (i % 2)) % n_z

    own = lax.dynamic_slice(hidden, (0, yl * half), (tok, half))
    other = lax.dynamic_slice(hidden, (0, (1 - yl) * half), (tok, half))
    theirs = swap(other, "yl", flip, 2)
    piece = half // 8
    index = ((1 - yl) * 8 + 2 * (z % 4) + c)[None].astype(jnp.int32)
    part = swap(cut(index, weights, piece), "yl", flip, 2)
    x_near, x_far, x_both = x ^ 1, last - x, last - (x ^ 1)

    def order(mine):
        a, b = (yl, 1 - yl) if mine else (1 - yl, yl)
        near, far = 2 * jnp.stack((x_near, x_both)), 2 * jnp.stack((x_far, x_both))
        own_near, own_far = 2 * jnp.stack((x, x_near)), 2 * jnp.stack((x, x_far))
        return [far + a, near + b, own_near + a, own_far + b]

    table = jnp.concatenate(order(True) + order(False)).astype(jnp.int32)
    mine, sent = ordered(table, (query_grad, key_grad, value_grad), tok)
    got = swap(sent, "yl", flip, 2)

    def gather(block):
        to_near = swap(block, "x", near, n_x)
        to_far = swap(block, "x", far, n_x)
        upper = swap(to_far[: tok // 2], "x", near, n_x)
        lower = swap(to_near[tok // 2 :], "x", far, n_x)
        return to_near, to_far, upper, lower

    a_near, a_far, a_upper, a_lower = gather(own)
    b_near, b_far, b_upper, b_lower = gather(theirs)
    tokens = joined(
        (a_far, a_upper, a_lower, b_near, b_upper, b_lower, own, a_near, theirs, b_far)
    )

    z_one = swap(part, "z", z_near, n_z)
    z_two = swap(part, "z", z_far, n_z)
    low, high = z_two[: piece // 2], z_one[piece // 2 :]
    low = swap(low, "z", z_near, n_z)
    high = swap(high, "z", z_far, n_z)
    pieces = joined((part, z_one, z_two, low, high))
    others = swap(pieces, "c", flip, 2)
    where = [(z, z_near(z), z_far(z), z + 2)[k] % 4 for k in range(4)]
    block = jnp.arange(4)
    slot = sum(k * (block == where[k]) for k in range(4))
    table = jnp.concatenate((yl * 4 + block, slot, c[None])).astype(jnp.int32)

    def plus(left, right):
        return (left.astype(F32) + right.astype(F32)).astype(BF16)

    def weight_part(grad):
        total = dot_rows(tokens, grad).astype(BF16).reshape(n_z, 2, tok, cols)
        give = lax.dynamic_index_in_dim(total, 1 - c, 1, keepdims=False)
        return total, swap(give, "c", flip, 2)

    mine_total, come_mine = weight_part(mine)
    theirs_total, come_theirs = weight_part(got)

    n_w = n_z // 2
    w, parity = z // 2, z % 2

    def w_near(i):
        return i ^ 2

    def w_far(i):
        return (i - 2 + 4 * (i // 2 % 2)) % n_z

    def ring(total, come, first):
        total = total.reshape(n_w, 2, 2, tok, cols)
        come = come.reshape(n_w, 2, tok, cols)

        def chunks(at, count, side):
            mine = lax.dynamic_slice(total, (at, side, c, 0, 0), (count, 1, 1, tok, cols))
            other = lax.dynamic_slice(come, (at, side, 0, 0), (count, 1, tok, cols))
            return mine[:, 0, 0].astype(F32) + other[:, 0].astype(F32)

        given = chunks(0, n_w, 1 - parity).astype(BF16)
        near = swap(given, "z", z_far if first else z_near, n_z)

        def chunk(step):
            forward = (w + step + first) % 2 == 0
            left = n_w - 1 - step
            to = jnp.where(forward, w + left, w - left + n_w) % n_w
            return chunks(to, 1, parity)[0] + lax.dynamic_index_in_dim(
                near, to, 0, keepdims=False
            ).astype(F32)

        passed = chunk(0).astype(BF16)
        for step in range(1, n_w):
            side = w_near if (step + first) % 2 else w_far
            taken = swap(passed, "z", side, n_z)
            passed = (taken.astype(F32) + chunk(step)).astype(BF16)
        return passed

    part_mine = ring(mine_total, come_mine, 0)
    part_theirs = ring(theirs_total, come_theirs, 1)

    args = (mine, got, weights, pieces, others)
    a_send, b_send = input_product(table, 0, *args)
    a_keep, b_keep = input_product(table, 1, *args)

    def pair_sum(keep, send, one, two):
        taken = swap(send, "x", one, n_x)
        mine, given = plus(keep[:tok], taken[:tok]), plus(keep[tok:], taken[tok:])
        taken = swap(given, "x", two, n_x)
        return plus(mine, taken)

    b_sum = pair_sum(b_keep, b_send, near, far)
    a_sum = pair_sum(a_keep, a_send, far, near)
    a_other = swap(b_sum, "yl", flip, 2)
    hidden_grad = jnp.where(
        yl == 0,
        jnp.concatenate((a_sum, a_other), axis=1),
        jnp.concatenate((a_other, a_sum), axis=1),
    )

    same = yh == yl
    first = jnp.where(same, part_mine, part_theirs)
    second = jnp.where(same, part_theirs, part_mine)
    home = [(2 * a + b, 2 * b + a) for a in range(2) for b in range(2)]
    away = [(2 * a + b, 2 * b + 1 - a) for a in range(2) for b in range(2)]
    first = lax.ppermute(first, ("yh", "yl"), home)
    second = lax.ppermute(second, ("yh", "yl"), away)
    weight_grad = first.astype(F32) + second.astype(F32)
    return (
        hidden_grad,
        weight_grad[:, :q_cols],
        weight_grad[:, q_cols : q_cols + k_cols],
        weight_grad[:, q_cols + k_cols :],
    )


def solution(mesh):
    torus = Mesh(mesh.devices.reshape(2, 8, 2, 4, 2), AXES)
    in_specs = (P(AXES, None),) + (P(DP, TP),) * 3 + (P(None, TP),) * 3
    out_specs = (P(AXES, None),) + (P(DP, TP),) * 3
    return jax.shard_map(body, mesh=torus, in_specs=in_specs, out_specs=out_specs, check_vma=False)
```

```python
import jax
import jax.numpy as jnp
from jax import lax
from jax.sharding import Mesh
from jax.sharding import PartitionSpec as P
from jax.experimental import pallas as pl
from jax.experimental.pallas import tpu as pltpu


AXES = ("yh", "z", "c", "x", "yl")
DP = ("yh", "z", "c")
TP = ("x", "yl")
BF16 = jnp.bfloat16
F32 = jnp.float32


def swap(value, axis, partner, size):
    return lax.ppermute(value, axis, [(i, partner(i)) for i in range(size)])


def flip(i):
    return i ^ 1


def sequential(**limits):
    return pltpu.CompilerParams(dimension_semantics=("arbitrary",), **limits)


def cut(index, weights, piece):
    widths = [w.shape[1] for w in weights]
    cols = sum(widths)

    def body(index, *refs):
        at = 0
        for ref, width in zip(refs[:-1], widths, strict=True):
            refs[-1][:, at : at + width] = ref[...]
            at += width

    return pl.pallas_call(
        body,
        name="cut",
        out_shape=jax.ShapeDtypeStruct((piece, cols), BF16),
        grid_spec=pltpu.PrefetchScalarGridSpec(
            num_scalar_prefetch=1,
            grid=(1,),
            in_specs=[pl.BlockSpec((piece, w), lambda i, t: (t[0], 0)) for w in widths],
            out_specs=pl.BlockSpec((piece, cols), lambda i, t: (0, 0)),
        ),
        compiler_params=sequential(),
    )(index, *weights)


def ordered(table, grads, tok):
    widths = [g.shape[1] for g in grads]
    cols = sum(widths)
    n_rows = grads[0].shape[0]
    steps = n_rows // tok

    def body(table, *refs):
        ins, outs = refs[:3], refs[3:]
        for i in range(2 * steps):
            row = pl.multiple_of(table[i] * tok, tok)
            at = 0
            for k, width in enumerate(widths):
                to = (i % steps) * tok
                outs[i // steps][to : to + tok, at : at + width] = ins[k][pl.ds(row, tok), :]
                at += width

    out = jax.ShapeDtypeStruct((n_rows, cols), BF16)
    return pl.pallas_call(
        body,
        name="ordered",
        out_shape=[out, out],
        grid_spec=pltpu.PrefetchScalarGridSpec(
            num_scalar_prefetch=1,
            grid=(1,),
            in_specs=[pl.BlockSpec(g.shape, lambda i, t: (0, 0)) for g in grads],
            out_specs=[pl.BlockSpec((n_rows, cols), lambda i, t: (0, 0))] * 2,
        ),
        compiler_params=sequential(),
    )(table, *grads)


def input_product(table, at, mine, got, weights, pieces, others):
    widths = [w.shape[1] for w in weights]
    cols = sum(widths)
    n_rows = mine.shape[0] // 2
    piece = pieces.shape[0] // 4
    steps = 4

    def body(table, mine, got, q, k, v, pieces, others, upper, lower):
        left = jnp.concatenate((q[...], k[...], v[...]), axis=1)
        south = table[2 * steps] == 0
        first = jnp.where(south, pieces[...], others[...])
        second = jnp.where(south, others[...], pieces[...])
        right = jnp.concatenate((first, second), axis=0)

        def times(a, b):
            return lax.dot_general(
                a[...], b, (((1,), (1,)), ((), ())), preferred_element_type=F32
            )

        total = (times(mine, left) + times(got, right)).astype(BF16)
        upper[...] = total[: n_rows // 2]
        lower[...] = total[n_rows // 2 :]

    row_spec = pl.BlockSpec((n_rows, cols), lambda i, t: (at, 0))
    piece_spec = pl.BlockSpec((piece, cols), lambda i, t: (t[steps + i], 0))
    return pl.pallas_call(
        body,
        out_shape=[jax.ShapeDtypeStruct((n_rows // 2, steps * 2 * piece), BF16)] * 2,
        grid_spec=pltpu.PrefetchScalarGridSpec(
            num_scalar_prefetch=1,
            grid=(steps,),
            in_specs=[row_spec, row_spec]
            + [pl.BlockSpec((2 * piece, w), lambda i, t: (t[i], 0)) for w in widths]
            + [piece_spec, piece_spec],
            out_specs=[pl.BlockSpec((n_rows // 2, 2 * piece), lambda i, t: (0, i))] * 2,
        ),
        compiler_params=sequential(),
        cost_estimate=pl.CostEstimate(
            flops=8 * n_rows * steps * piece * cols,
            bytes_accessed=8 * steps * piece * cols,
            transcendentals=0,
        ),
    )(table, mine, got, *weights, pieces, others)


def dot_rows(left, right):
    return lax.dot_general(left, right, (((0,), (0,)), ((), ())), preferred_element_type=F32)


def joined(arrays):
    return jnp.concatenate(arrays, axis=0)


def body(hidden, query_grad, key_grad, value_grad, w_query, w_key, w_value):
    n_x = lax.axis_size("x")
    n_z = lax.axis_size("z")
    yl = lax.axis_index("yl")
    yh = lax.axis_index("yh")
    x = lax.axis_index("x")
    c = lax.axis_index("c")
    z = lax.axis_index("z")
    tok, width = hidden.shape
    half = width // 2
    q_cols, k_cols = w_query.shape[1], w_key.shape[1]
    cols = q_cols + 2 * k_cols
    last = n_x - 1
    weights = (w_query, w_key, w_value)

    def near(i):
        return i ^ 1

    def far(i):
        return last - i

    def z_near(i):
        return i ^ 1

    def z_far(i):
        return (i - 1 + 2 * (i % 2)) % n_z

    own = lax.dynamic_slice(hidden, (0, yl * half), (tok, half))
    other = lax.dynamic_slice(hidden, (0, (1 - yl) * half), (tok, half))
    theirs = swap(other, "yl", flip, 2)
    piece = half // 8
    index = ((1 - yl) * 8 + 2 * (z % 4) + c)[None].astype(jnp.int32)
    part = swap(cut(index, weights, piece), "yl", flip, 2)
    x_near, x_far, x_both = x ^ 1, last - x, last - (x ^ 1)

    def order(mine):
        a, b = (yl, 1 - yl) if mine else (1 - yl, yl)
        near, far = 2 * jnp.stack((x_near, x_both)), 2 * jnp.stack((x_far, x_both))
        own_near, own_far = 2 * jnp.stack((x, x_near)), 2 * jnp.stack((x, x_far))
        return [far + a, near + b, own_near + a, own_far + b]

    table = jnp.concatenate(order(True) + order(False)).astype(jnp.int32)
    mine, sent = ordered(table, (query_grad, key_grad, value_grad), tok)
    got = swap(sent, "yl", flip, 2)

    def gather(block):
        to_near = swap(block, "x", near, n_x)
        to_far = swap(block, "x", far, n_x)
        upper = swap(to_far[: tok // 2], "x", near, n_x)
        lower = swap(to_near[tok // 2 :], "x", far, n_x)
        return to_near, to_far, upper, lower

    a_near, a_far, a_upper, a_lower = gather(own)
    b_near, b_far, b_upper, b_lower = gather(theirs)
    tokens = joined(
        (a_far, a_upper, a_lower, b_near, b_upper, b_lower, own, a_near, theirs, b_far)
    )

    z_one = swap(part, "z", z_near, n_z)
    z_two = swap(part, "z", z_far, n_z)
    low, high = z_two[: piece // 2], z_one[piece // 2 :]
    low = swap(low, "z", z_near, n_z)
    high = swap(high, "z", z_far, n_z)
    pieces = joined((part, z_one, z_two, low, high))
    others = swap(pieces, "c", flip, 2)
    where = [(z, z_near(z), z_far(z), z + 2)[k] % 4 for k in range(4)]
    block = jnp.arange(4)
    slot = sum(k * (block == where[k]) for k in range(4))
    table = jnp.concatenate((yl * 4 + block, slot, c[None])).astype(jnp.int32)

    def plus(left, right):
        return (left.astype(F32) + right.astype(F32)).astype(BF16)

    def weight_part(grad):
        total = dot_rows(tokens, grad).astype(BF16).reshape(n_z, 2, tok, cols)
        give = lax.dynamic_index_in_dim(total, 1 - c, 1, keepdims=False)
        return total, swap(give, "c", flip, 2)

    mine_total, come_mine = weight_part(mine)
    theirs_total, come_theirs = weight_part(got)

    n_w = n_z // 2
    w, parity = z // 2, z % 2

    def w_near(i):
        return i ^ 2

    def w_far(i):
        return (i - 2 + 4 * (i // 2 % 2)) % n_z

    def ring(total, come, first):
        total = total.reshape(n_w, 2, 2, tok, cols)
        come = come.reshape(n_w, 2, tok, cols)

        def chunks(at, count, side):
            mine = lax.dynamic_slice(total, (at, side, c, 0, 0), (count, 1, 1, tok, cols))
            other = lax.dynamic_slice(come, (at, side, 0, 0), (count, 1, tok, cols))
            return mine[:, 0, 0].astype(F32) + other[:, 0].astype(F32)

        given = chunks(0, n_w, 1 - parity).astype(BF16)
        near = swap(given, "z", z_far if first else z_near, n_z)

        def chunk(step):
            forward = (w + step + first) % 2 == 0
            left = n_w - 1 - step
            to = jnp.where(forward, w + left, w - left + n_w) % n_w
            return chunks(to, 1, parity)[0] + lax.dynamic_index_in_dim(
                near, to, 0, keepdims=False
            ).astype(F32)

        passed = chunk(0).astype(BF16)
        for step in range(1, n_w):
            side = w_near if (step + first) % 2 else w_far
            taken = swap(passed, "z", side, n_z)
            passed = (taken.astype(F32) + chunk(step)).astype(BF16)
        return passed

    part_mine = ring(mine_total, come_mine, 0)
    part_theirs = ring(theirs_total, come_theirs, 1)

    args = (mine, got, weights, pieces, others)
    a_send, b_send = input_product(table, 0, *args)
    a_keep, b_keep = input_product(table, 1, *args)

    def pair_sum(keep, send, one, two):
        taken = swap(send, "x", one, n_x)
        mine, given = plus(keep[:tok], taken[:tok]), plus(keep[tok:], taken[tok:])
        taken = swap(given, "x", two, n_x)
        return plus(mine, taken)

    b_sum = pair_sum(b_keep, b_send, near, far)
    a_sum = pair_sum(a_keep, a_send, far, near)
    a_other = swap(b_sum, "yl", flip, 2)
    hidden_grad = jnp.where(
        yl == 0,
        jnp.concatenate((a_sum, a_other), axis=1),
        jnp.concatenate((a_other, a_sum), axis=1),
    )

    same = yh == yl
    first = jnp.where(same, part_mine, part_theirs)
    second = jnp.where(same, part_theirs, part_mine)
    home = [(2 * a + b, 2 * b + a) for a in range(2) for b in range(2)]
    away = [(2 * a + b, 2 * b + 1 - a) for a in range(2) for b in range(2)]
    first = lax.ppermute(first, ("yh", "yl"), home)
    second = lax.ppermute(second, ("yh", "yl"), away)

    def added(start, width):
        left, right = first[:, start : start + width], second[:, start : start + width]
        return left.astype(F32) + right.astype(F32)

    return (
        hidden_grad,
        added(0, q_cols),
        added(q_cols, k_cols),
        added(q_cols + k_cols, k_cols),
    )


def solution(mesh):
    torus = Mesh(mesh.devices.reshape(2, 8, 2, 4, 2), AXES)
    in_specs = (P(AXES, None),) + (P(DP, TP),) * 3 + (P(None, TP),) * 3
    out_specs = (P(AXES, None),) + (P(DP, TP),) * 3
    return jax.shard_map(body, mesh=torus, in_specs=in_specs, out_specs=out_specs, check_vma=False)
```
